32 devices in a mesh: rve: 4 (over y, x), slab: 8 (over z, core).
Axes of the slice: x: 2, y: 2, z: 4, core: 2. Of those that a mesh axis runs over, the one named last changes fastest.
Arguments:
- displacement: float32 [32, 3, 128, 256], P('slab', None, 'rve'), parts along dimension 2, may hold values from -6 to 6
- load: float32 [32, 3, 128, 256], P('slab', None, 'rve'), parts along dimension 2, may hold values from -24 to 24
- phase: int32 [32, 128, 256], P('slab', 'rve'), parts along dimension 1, may hold values from 0 to 2
- moduli: float32 [2, 3], replicated, may hold values from 0.5 to 4
Outputs:
- solution: float32 [32, 3, 128, 256], P('slab', None, 'rve'), parts along dimension 2
- residual: float32 [32, 3, 128, 256], P('slab', None, 'rve'), parts along dimension 2
The draws below stay inside these ranges and needn't reach their ends.
There are 4 independent parts, one for each index of `rve`. The reference program is written for one: setup_inputs(seed, part) draws one part's arguments, and reference() takes and returns one part's arrays. A program takes and returns all parts, laid end to end along the dimension named above; an argument that names none is the same for every part. Nothing has to cross between parts.
All inputs are finite; a program needn't handle non-finite values.
Results may differ from the reference program's by a relative error of at most 0.00002.
Values sent between devices are 32-bit elements; how exact they have to be, the bound alone decides.
A program may use at most 64 MiB of HBM per device.

```python
import math
import jax
import jax.numpy as jnp

NX = 32
NY = 256
PHASES = 3
SWEEPS = 6
NZ = 32


def place_ends(result, key, least, largest):
    dims = result.shape
    index_at = [jax.random.randint(jax.random.fold_in(key, axis), (), 0, dims[axis]) for axis in range(len(dims))]
    result = result.at[tuple(index_at)].set(least)
    longest = dims.index(max(dims))
    index_at[longest] = (index_at[longest] + 1) % dims[longest]
    return result.at[tuple(index_at)].set(largest)


def level_of(key, extent, shards, least, largest):
    loudness, own = 1.0, jax.random.fold_in(key, 6)
    for axis_at, shards_of in shards:
        heights = jnp.exp(jax.random.uniform(jax.random.fold_in(own, axis_at), (shards_of,), jnp.float32, least / len(shards), largest / len(shards)))
        loudness = loudness * jnp.repeat(heights, extent[axis_at] // shards_of).reshape([-1 if axis == axis_at else 1 for axis in range(len(extent))])
    return loudness


def gaussian(own_key, shape, scale, reach, cuts=(), kind=jnp.bfloat16):
    result = scale * jax.random.normal(own_key, shape, jnp.float32)
    if cuts:
        result = result * level_of(own_key, shape, cuts, -0.22, 0.18)
    return jnp.clip(result, -reach, reach).astype(kind)


def setup_inputs(seed: int = 0, part: int = 0) -> dict:
    streams_of = jax.random.split(jax.random.key(seed), 5)
    part_keys = jax.random.split(jax.random.fold_in(streams_of[4], part), 5)
    return {
        "displacement": gaussian(part_keys[0], (NZ, 3, NX, NY), 1.0, 6.0, ((0, 8),), jnp.float32),
        "load": gaussian(part_keys[1], (NZ, 3, NX, NY), 4.0, 24.0, ((0, 8),), jnp.float32),
        "phase": place_ends(jax.random.randint(part_keys[2], (NZ, NX, NY), 0, PHASES), jax.random.fold_in(part_keys[2], 1), 0, PHASES - 1).astype(jnp.int32),
        "moduli": jnp.clip(jnp.exp(jax.random.uniform(streams_of[3], (2, PHASES), jnp.float32, math.log(0.5), math.log(4.0))), 0.5, 4.0),
    }


def plus_next(value, axis):
    return value + jnp.roll(value, -1, axis)


def minus_next(value, axis):
    return jnp.roll(value, -1, axis) - value


def plus_prev(value, axis):
    return value + jnp.roll(value, 1, axis)


def prev_minus(value, axis):
    return jnp.roll(value, 1, axis) - value


def materials(phase, moduli):
    lame = jnp.zeros(phase.shape, jnp.float32)
    shear = jnp.zeros(phase.shape, jnp.float32)
    for index in range(moduli.shape[1]):
        select = (phase == index).astype(jnp.float32)
        lame = lame + select * moduli[0, index]
        shear = shear + select * moduli[1, index]
    return lame, shear


def element_terms(lower, upper, lame, shear):
    total = lower + upper
    jump = upper - lower
    grad_x = 0.25 * minus_next(plus_next(total, -1), -2)
    grad_y = 0.25 * plus_next(minus_next(total, -1), -2)
    grad_z = 0.25 * plus_next(plus_next(jump, -1), -2)
    trace = grad_x[:, 0] + grad_y[:, 1] + grad_z[:, 2]
    normal_x = lame * trace + 2.0 * shear * grad_x[:, 0]
    normal_y = lame * trace + 2.0 * shear * grad_y[:, 1]
    normal_z = lame * trace + 2.0 * shear * grad_z[:, 2]
    shear_xy = shear * (grad_y[:, 0] + grad_x[:, 1])
    shear_xz = shear * (grad_z[:, 0] + grad_x[:, 2])
    shear_yz = shear * (grad_z[:, 1] + grad_y[:, 2])
    col_x = jnp.stack([normal_x, shear_xy, shear_xz], 1)
    col_y = jnp.stack([shear_xy, normal_y, shear_yz], 1)
    col_z = jnp.stack([shear_xz, shear_yz, normal_z], 1)
    inplane = 0.25 * (plus_prev(prev_minus(col_x, -2), -1) + plus_prev(prev_minus(col_y, -1), -2))
    vertical = 0.25 * plus_prev(plus_prev(col_z, -1), -2)
    return inplane, vertical


def operate(field, lame, shear):
    inplane, vertical = element_terms(field, jnp.roll(field, -1, 0), lame, shear)
    return inplane + jnp.roll(inplane, 1, 0) + jnp.roll(vertical, 1, 0) - vertical


def reference(displacement, load, phase, moduli):
    lame, shear = materials(phase, moduli)
    stiff = lame + 4.0 * shear
    diagonal = plus_prev(plus_prev(plus_prev(stiff, -1), -2), 0) / 16.0
    diagonal = diagonal[:, None]
    field = displacement
    for sweep in range(SWEEPS):
        field = field + 0.5 * (load - operate(field, lame, shear)) / diagonal
    return field, load - operate(field, lame, shear)
```

```python
import functools

import jax
import jax.numpy as jnp
from jax import lax
from jax.experimental import pallas as pl
from jax.experimental.pallas import tpu as pltpu
from jax.sharding import PartitionSpec as P

SWEEPS = 6
MESH = pl.DeviceIdType.MESH
ROWS = 8

STRESS = ((0, 3, 4), (3, 1, 5), (4, 5, 2))


def shift_next(value, axis):
    return pltpu.roll(value, value.shape[axis] - 1, axis)


def shift_prev(value, axis):
    return pltpu.roll(value, 1, axis)


def kernel(
    peers, disp, load, phase, moduli, out, rest,
    raw, u, ld, ph, lam, mu, mu2, inv, fwd, st, near, held, pull,
    in_sem, out_send, out_recv, in_send, in_recv,
):
    local, _, nx, ny = disp.shape
    phases = moduli.shape[1]
    me = lax.axis_index("slab")
    odd = lax.rem(me, 2)
    sign = (1 - 2 * odd).astype(jnp.float32)
    outer = lax.rem(me + 2 * odd - 1 + peers, peers)
    inner = me + 1 - 2 * odd

    def plane(p):
        return jnp.where(odd == 1, local - 1 - p, p)

    loads = []

    def bring(src, dst):
        copy = pltpu.make_async_copy(src, dst, in_sem.at[len(loads)])
        loads.append(copy)
        copy.start()
        return copy

    order = [0, local - 1] + list(range(1, local - 1))
    nodes = {p: bring(disp.at[plane(p)], raw.at[p + 1]) for p in order[:2]}
    kinds = [bring(phase.at[k], ph.at[jnp.where(odd == 1, local - k, k + 2)]) for k in range(local)]
    nodes.update({p: bring(disp.at[plane(p)], raw.at[p + 1]) for p in order[2:]})
    bases = [bring(load.at[plane(p)], ld.at[p]) for p in range(local)]

    barrier = pltpu.get_barrier_semaphore()
    for peer in (outer, inner):
        pl.semaphore_signal(barrier, inc=1, device_id={"slab": peer}, device_id_type=MESH)
    pl.semaphore_wait(barrier, 2)

    def remote(src, dst, sends, recvs, at, peer):
        return pltpu.make_async_remote_copy(
            src_ref=src, dst_ref=dst, send_sem=sends.at[at], recv_sem=recvs.at[at],
            device_id={"slab": peer}, device_id_type=MESH,
        )

    out_copy = functools.partial(remote, sends=out_send, recvs=out_recv, peer=outer)
    in_copy = functools.partial(remote, sends=in_send, recvs=in_recv, peer=inner)
    out_node = out_copy(raw.at[1], raw.at[0], at=SWEEPS)
    out_far = out_copy(ph.at[2], ph.at[0], at=SWEEPS + 1)
    out_near = out_copy(ph.at[1], ph.at[1], at=SWEEPS + 2)
    in_kind = in_copy(ph.at[local + 1], ph.at[local + 1], at=SWEEPS + 1)
    pulls = [out_copy(held.at[s], pull.at[s], at=s) for s in range(SWEEPS)]

    def at_level(s, p):
        return raw.at[p + 1] if s == 0 else u.at[s - 1, p + 1]

    inners = [in_copy(at_level(s, local - 1), at_level(s, local), at=s) for s in range(SWEEPS + 1)]

    nodes[0].wait()
    out_node.start()
    nodes[local - 1].wait()
    inners[0].start()
    for copy in kinds:
        copy.wait()

    @pl.when(odd == 1)
    def _():
        out_near.start()

    @pl.when(odd == 0)
    def _():
        in_kind.start()

    def value_at(s, p, c):
        value = at_level(s, p)[c]
        if c == 2 and s == 0:
            return value * sign
        if c == 2 and p == local:
            return -value
        return value

    def material(e):
        for r in range(0, nx, ROWS):
            at = pl.ds(r, ROWS)
            kind = ph[e + 2, at, :]
            lame = jnp.zeros(kind.shape, jnp.float32)
            shear = jnp.zeros(kind.shape, jnp.float32)
            for index in range(phases):
                lame = jnp.where(kind == index, moduli[0, index] * 0.0625, lame)
                shear = jnp.where(kind == index, moduli[1, index] * 0.0625, shear)
            lam[e + 2, at, :] = lame
            mu[e + 2, at, :] = shear
            mu2[e + 2, at, :] = shear + shear

    def diagonal(p):
        total = (lam[p + 1] + 2.0 * mu2[p + 1]) + (lam[p + 2] + 2.0 * mu2[p + 2])
        total = total + shift_prev(total, 1)
        total = total + shift_prev(total, 0)
        inv[p + 1] = 0.5 / total

    def forward(s, p):
        for c in range(3):
            value = value_at(s, p, c)
            moved = shift_next(value, 1)
            total, jump = value + moved, moved - value
            moved = shift_next(total, 0)
            fwd[p + 1, c] = moved - total
            fwd[p + 1, 6 + c] = moved + total
            fwd[p + 1, 3 + c] = jump + shift_next(jump, 0)

    def element(e, half=False, into=None):
        lo, hi = e + 1, e + 2
        to = e + 2 if into is None else into
        for r in range(0, nx, ROWS):
            at = pl.ds(r, ROWS)
            gx, gy, gz = ([fwd[hi, 3 * a + c, at, :] for c in range(3)] for a in range(3))
            if not half:
                gx = [gx[c] + fwd[lo, c, at, :] for c in range(3)]
                gy = [gy[c] + fwd[lo, 3 + c, at, :] for c in range(3)]
                gz = [gz[c] - fwd[lo, 6 + c, at, :] for c in range(3)]
            bulk = lam[e + 2, at, :] * (gx[0] + gy[1] + gz[2])
            two, one = mu2[e + 2, at, :], mu[e + 2, at, :]
            st[to, 0, at, :] = bulk + two * gx[0]
            st[to, 1, at, :] = bulk + two * gy[1]
            st[to, 2, at, :] = bulk + two * gz[2]
            st[to, 3, at, :] = one * (gy[0] + gx[1])
            st[to, 4, at, :] = one * (gz[0] + gx[2])
            st[to, 5, at, :] = one * (gz[1] + gy[2])

    def force(px, qy, rz):
        e = (rz - px) + shift_prev(rz + px, 0)
        b = qy + shift_prev(qy, 0)
        return (e - b) + shift_prev(e + b, 1)

    def internal(p, c):
        lo, hi = p + 1, p + 2
        x, y, z = STRESS[c]
        return force(st[lo, x] + st[hi, x], st[lo, y] + st[hi, y], st[lo, z] - st[hi, z])

    def based(p, c):
        return ld[p, c] * sign if c == 2 else ld[p, c]

    def settle(s, p, c, value):
        u[s - 1, p + 1, c] = value
        if s == SWEEPS and 0 <= p < local:
            out[plane(p), c] = value * sign if c == 2 else value

    def advance(s, p):
        for c in range(3):
            remain = based(p, c) - internal(p, c)
            if s > SWEEPS:
                rest[plane(p), c] = remain * sign if c == 2 else remain
            else:
                settle(s, p, c, value_at(s - 1, p, c) + inv[p + 1] * remain)

    def prepare(s):
        element(-2, half=True)
        for c in range(3):
            near[c] = value_at(s - 1, -1, c) - inv[0] * internal(-1, c)

    def land(s):
        for c in range(3):
            drawn = inv[0] * pull[s - 1, c]
            settle(s, -1, c, near[c] - drawn if c == 2 else near[c] + drawn)

    spare = local + 2

    def offer(s):
        element(0, half=True, into=spare)
        for c in range(3):
            x, y, z = STRESS[c]
            held[s, c] = based(0, c) - force(st[spare, x], st[spare, y], -st[spare, z])
        pulls[s].start()

    def outer_part(t):
        if t == -1:
            out_node.wait_recv()

            @pl.when(odd == 0)
            def _():
                out_near.wait_recv()

            material(-1)
            diagonal(0)
        if 0 <= t < SWEEPS:
            pulls[t].wait_recv()
            land(t + 1)
        if -1 <= t < SWEEPS:
            forward(t + 1, -1)
            element(-1)
            advance(t + 2, 0)

    def middle_part(t):
        if 0 <= t + 2 <= SWEEPS:
            forward(t + 2, 0)
            element(0)
            advance(t + 3, 1)

    def offer_part(t):
        if 0 <= t + 3 <= SWEEPS:
            forward(t + 3, 1)
        if 0 <= t + 3 < SWEEPS:
            offer(t + 3)

    def inner_part(t):
        for p in range(2, local):
            if 0 <= t + p + 1 <= SWEEPS:
                if p > 2:
                    forward(t + p + 1, p - 1)
                element(p - 1)
                if p == local - 1:
                    inners[t + p + 1].wait_recv()
                    if t + p + 1 == 0:

                        @pl.when(odd == 1)
                        def _():
                            in_kind.wait_recv()

                        material(local - 1)
                        diagonal(local - 1)
                    forward(t + p + 1, local)
                    element(local - 1)
                advance(t + p + 2, p)
                if p == local - 1 and t + p + 2 <= SWEEPS:
                    inners[t + p + 2].start()
        if 0 <= t + local + 1 <= SWEEPS:
            forward(t + local + 1, local - 1)

    def after_part(t):
        if t == -1:
            out_far.wait_recv()
            material(-2)
            diagonal(-1)
        if -1 <= t < SWEEPS - 1:
            prepare(t + 2)

    for p in range(local - 1):
        material(p)
    for p in range(1, local - 1):
        diagonal(p)
    for copy in [nodes[p] for p in order[2:]] + bases:
        copy.wait()
    for t in range(-local - 1, SWEEPS):
        outer_part(t)
        middle_part(t)
        offer_part(t)
        if t == -3:
            out_far.start()
        inner_part(t)
        after_part(t)

    out_node.wait_send()
    out_far.wait_send()

    @pl.when(odd == 1)
    def _():
        out_near.wait_send()

    @pl.when(odd == 0)
    def _():
        in_kind.wait_send()

    for copy in pulls + inners:
        copy.wait_send()


def write_out(field, remain, out, rest, sem):
    copies = [pltpu.make_async_copy(field, out, sem.at[0]), pltpu.make_async_copy(remain, rest, sem.at[1])]
    for copy in copies:
        copy.start()
    for copy in copies:
        copy.wait()


def on_device(peers, displacement, load, phase, moduli):
    local, comps, nx, ny = displacement.shape
    plane = (nx, ny)
    hbm = pl.BlockSpec(memory_space=pl.ANY)
    f32 = jnp.float32
    vmem = pl.BlockSpec(memory_space=pltpu.VMEM)
    held = pl.pallas_call(
        functools.partial(kernel, peers),
        out_shape=[pltpu.VMEM(displacement.shape, f32)] * 2,
        in_specs=[hbm, hbm, hbm, pl.BlockSpec(memory_space=pltpu.SMEM)],
        out_specs=[vmem, vmem],
        scratch_shapes=[
            pltpu.VMEM((local + 2, comps) + plane, f32),
            pltpu.VMEM((SWEEPS, local + 2, comps) + plane, f32),
            pltpu.VMEM((local, comps) + plane, f32),
            pltpu.VMEM((local + 2,) + plane, jnp.int32),
            pltpu.VMEM((local + 2,) + plane, f32),
            pltpu.VMEM((local + 2,) + plane, f32),
            pltpu.VMEM((local + 2,) + plane, f32),
            pltpu.VMEM((local + 1,) + plane, f32),
            pltpu.VMEM((local + 2, 9) + plane, f32),
            pltpu.VMEM((local + 3, 6) + plane, f32),
            pltpu.VMEM((comps,) + plane, f32),
            pltpu.VMEM((SWEEPS, comps) + plane, f32),
            pltpu.VMEM((SWEEPS, comps) + plane, f32),
            pltpu.SemaphoreType.DMA((3 * local,)),
            pltpu.SemaphoreType.DMA((SWEEPS + 3,)),
            pltpu.SemaphoreType.DMA((SWEEPS + 3,)),
            pltpu.SemaphoreType.DMA((SWEEPS + 2,)),
            pltpu.SemaphoreType.DMA((SWEEPS + 2,)),
        ],
        compiler_params=pltpu.CompilerParams(collective_id=0, has_side_effects=True),
    )(displacement, load, phase, moduli)
    return pl.pallas_call(
        write_out,
        out_shape=[jax.ShapeDtypeStruct(displacement.shape, f32)] * 2,
        in_specs=[hbm, hbm],
        out_specs=[hbm, hbm],
        scratch_shapes=[pltpu.SemaphoreType.DMA((2,))],
    )(*[pltpu.with_memory_space_constraint(one, pltpu.VMEM) for one in held])


def solution(mesh):
    in_specs = (
        P("slab", None, "rve", None),
        P("slab", None, "rve", None),
        P("slab", "rve", None),
        P(),
    )
    out_specs = (P("slab", None, "rve", None), P("slab", None, "rve", None))
    return jax.shard_map(
        functools.partial(on_device, mesh.shape["slab"]),
        mesh=mesh, in_specs=in_specs, out_specs=out_specs, check_vma=False,
    )
```

```python
import functools

import jax
import jax.numpy as jnp
from jax import lax
from jax.experimental import pallas as pl
from jax.experimental.pallas import tpu as pltpu
from jax.sharding import PartitionSpec as P

SWEEPS = 6
MESH = pl.DeviceIdType.MESH
ROWS = 8

STRESS = ((0, 3, 4), (3, 1, 5), (4, 5, 2))


def shift_next(value, axis):
    return pltpu.roll(value, value.shape[axis] - 1, axis)


def shift_prev(value, axis):
    return pltpu.roll(value, 1, axis)


def slopes(value):
    moved = shift_next(value, 1)
    total, jump = value + moved, moved - value
    moved = shift_next(total, 0)
    return moved - total, jump + shift_next(jump, 0), moved + total


def stresses(gx, gy, gz, lam, mu, mu2):
    bulk = lam * (gx[0] + gy[1] + gz[2])
    return (
        bulk + mu2 * gx[0], bulk + mu2 * gy[1], bulk + mu2 * gz[2],
        mu * (gy[0] + gx[1]), mu * (gz[0] + gx[2]), mu * (gz[1] + gy[2]),
    )


def force(px, qy, rz):
    e = (rz - px) + shift_prev(rz + px, 0)
    b = qy + shift_prev(qy, 0)
    return (e - b) + shift_prev(e + b, 1)


def plane_of(odd, local, p):
    return jnp.where(odd == 1, local - 1 - p, p)


def kernel(
    peers, disp, load, phase, table, out, rest, rim_u, rim_m,
    moduli, raw, u, ld, ph, lam, mu, mu2, inv, fwd, st, near, held, pull,
    in_sem, send_sem, recv_sem,
):
    local, _, nx, ny = disp.shape
    phases = table.shape[1]
    me = lax.axis_index("slab")
    odd = lax.rem(me, 2)
    closing = jnp.logical_or(me == 0, me == peers - 1)
    sign = (1 - 2 * odd).astype(jnp.float32)
    outer = lax.rem(me + 2 * odd - 1 + peers, peers)
    inner = me + 1 - 2 * odd

    def plane(p):
        return plane_of(odd, local, p)

    def bring(src, dst, at):
        return pltpu.make_async_copy(src, dst, in_sem.at[at])

    def bring_node(p, at):
        return bring(disp.at[plane(p)], raw.at[p + 1], at)

    rim, hub, consts = bring_node(0, 0), bring_node(local - 1, 1), bring(table, moduli, 2)
    kinds = bring(phase, ph.at[pl.ds(2, local)], 3)
    middles = bring(disp.at[pl.ds(1, local - 2)], raw.at[pl.ds(2, local - 2)], 4)
    bases = bring(load, ld, 5)
    rim.start()
    hub.start()
    for k in range(local):
        bring(phase.at[k], ph.at[jnp.where(odd == 1, local - k, k + 2)], 3).start()
    consts.start()
    for p in range(1, local - 1):
        bring_node(p, 4).start()
    for p in range(local):
        bring(load.at[plane(p)], ld.at[p], 5).start()

    barrier = pltpu.get_barrier_semaphore()
    for peer in (outer, inner):
        pl.semaphore_signal(barrier, inc=1, device_id={"slab": peer}, device_id_type=MESH)
    pl.semaphore_wait(barrier, 2)

    def remote(src, dst, send, recv, peer):
        return pltpu.make_async_remote_copy(
            src_ref=src, dst_ref=dst, send_sem=send_sem.at[send], recv_sem=recv_sem.at[recv],
            device_id={"slab": peer}, device_id_type=MESH,
        )

    out_node = remote(raw.at[1], raw.at[0], 2, SWEEPS, outer)
    out_far = remote(ph.at[2], ph.at[0], 3, SWEEPS + 1, outer)
    out_near = remote(ph.at[1], ph.at[1], 4, SWEEPS + 2, outer)
    in_kind = remote(ph.at[local + 1], ph.at[local + 1], 4, SWEEPS + 2, inner)
    pulls = [remote(held.at[s], pull.at[s], 0, s, outer) for s in range(SWEEPS)]

    def at_level(s, p):
        return raw.at[p + 1] if s == 0 else u.at[s - 1, p + 1]

    inners = [
        remote(at_level(s, local - 1), at_level(s, local), 1 if s else 5, SWEEPS + 3 + s % 2, inner)
        for s in range(SWEEPS + 1)
    ]

    rim.wait()
    out_node.start()
    hub.wait()
    inners[0].start()
    kinds.wait()

    @pl.when(odd == 1)
    def _():
        out_near.start()

    @pl.when(odd == 0)
    def _():
        in_kind.start()

    out_far.start()

    def value_at(s, p, c):
        value = at_level(s, p)[c]
        if c == 2 and s == 0:
            return value * sign
        if c == 2 and p == local:
            return -value
        return value

    def material(e):
        for r in range(0, nx, ROWS):
            at = pl.ds(r, ROWS)
            kind = ph[e + 2, at, :]
            lame = jnp.zeros(kind.shape, jnp.float32)
            shear = jnp.zeros(kind.shape, jnp.float32)
            for index in range(phases):
                lame = jnp.where(kind == index, moduli[0, index] * 0.0625, lame)
                shear = jnp.where(kind == index, moduli[1, index] * 0.0625, shear)
            lam[e + 2, at, :] = lame
            mu[e + 2, at, :] = shear
            mu2[e + 2, at, :] = shear + shear

    def diagonal(p):
        total = (lam[p + 1] + 2.0 * mu2[p + 1]) + (lam[p + 2] + 2.0 * mu2[p + 2])
        total = total + shift_prev(total, 1)
        total = total + shift_prev(total, 0)
        inv[p + 1] = 0.5 / total

    def forward(s, p):
        for c in range(3):
            x, y, z = slopes(value_at(s, p, c))
            fwd[p + 1, c], fwd[p + 1, 3 + c], fwd[p + 1, 6 + c] = x, y, z

    def element(e, half=False, into=None):
        lo, hi = e + 1, e + 2
        to = e + 2 if into is None else into
        for r in range(0, nx, ROWS):
            at = pl.ds(r, ROWS)
            gx, gy, gz = ([fwd[hi, 3 * a + c, at, :] for c in range(3)] for a in range(3))
            if not half:
                gx = [gx[c] + fwd[lo, c, at, :] for c in range(3)]
                gy = [gy[c] + fwd[lo, 3 + c, at, :] for c in range(3)]
                gz = [gz[c] - fwd[lo, 6 + c, at, :] for c in range(3)]
            made = stresses(gx, gy, gz, lam[e + 2, at, :], mu[e + 2, at, :], mu2[e + 2, at, :])
            for k in range(6):
                st[to, k, at, :] = made[k]

    def internal(p, c):
        lo, hi = p + 1, p + 2
        x, y, z = STRESS[c]
        return force(st[lo, x] + st[hi, x], st[lo, y] + st[hi, y], st[lo, z] - st[hi, z])

    def based(p, c):
        return ld[p, c] * sign if c == 2 else ld[p, c]

    def settle(s, p, c, value):
        if p < 0 and s == SWEEPS:
            rim_u[c] = value
            return
        u[s - 1, p + 1, c] = value
        if s == SWEEPS and 0 <= p < local:
            out[plane(p), c] = value * sign if c == 2 else value

    def advance(s, p):
        for c in range(3):
            remain = based(p, c) - internal(p, c)
            if s > SWEEPS:
                rest[plane(p), c] = remain * sign if c == 2 else remain
            else:
                settle(s, p, c, value_at(s - 1, p, c) + inv[p + 1] * remain)

    def prepare(s):
        element(-2, half=True)
        for c in range(3):
            near[c] = value_at(s - 1, -1, c) - inv[0] * internal(-1, c)

    def land(s):
        for c in range(3):
            drawn = inv[0] * pull[s - 1, c]
            settle(s, -1, c, near[c] - drawn if c == 2 else near[c] + drawn)

    spare = local + 2

    def offer(s):
        element(0, half=True, into=spare)
        for c in range(3):
            x, y, z = STRESS[c]
            held[s, c] = based(0, c) - force(st[spare, x], st[spare, y], -st[spare, z])
        if s < SWEEPS - 1:
            pulls[s].start()
        else:
            pl.when(closing)(pulls[s].start)

    def leave():
        element(-1, half=True)
        for c in range(3):
            remain = based(0, c) - internal(0, c)
            rest[plane(0), c] = remain * sign if c == 2 else remain
        for k, field in enumerate((lam, mu, mu2)):
            rim_m[k] = field[1]

    def outer_part(t):
        if t == -1:
            out_node.wait_recv()

            @pl.when(odd == 0)
            def _():
                out_near.wait_recv()

            material(-1)
            diagonal(0)
        if 0 <= t < SWEEPS:
            pulls[t].wait_recv()
            land(t + 1)
        if -1 <= t < SWEEPS - 1:
            forward(t + 1, -1)
            element(-1)
            advance(t + 2, 0)
            if t == SWEEPS - 3:
                pl.when(jnp.logical_not(closing))(pulls[SWEEPS - 1].start)

    def middle_part(t):
        if 0 <= t + 2 <= SWEEPS:
            forward(t + 2, 0)
            element(0)
            advance(t + 3, 1)

    def offer_part(t):
        if 0 <= t + 3 <= SWEEPS:
            forward(t + 3, 1)
        if 0 <= t + 3 < SWEEPS:
            offer(t + 3)

    def inner_part(t):
        for p in range(2, local):
            if 0 <= t + p + 1 <= SWEEPS:
                if p > 2:
                    forward(t + p + 1, p - 1)
                element(p - 1)
                if p == local - 1:
                    inners[t + p + 1].wait_recv()
                    if t + p + 1 == 0:

                        @pl.when(odd == 1)
                        def _():
                            in_kind.wait_recv()

                        material(local - 1)
                        diagonal(local - 1)
                    forward(t + p + 1, local)
                    element(local - 1)
                advance(t + p + 2, p)
                if p == local - 1 and t + p + 2 <= SWEEPS:
                    inners[t + p + 2].start()
        if 0 <= t + local + 1 <= SWEEPS:
            forward(t + local + 1, local - 1)

    def after_part(t):
        if t == -1:
            out_far.wait_recv()
            material(-2)
            diagonal(-1)
        if -1 <= t < SWEEPS - 1:
            prepare(t + 2)
        if t == SWEEPS - 2:
            leave()

    consts.wait()
    for p in range(local - 1):
        material(p)
    for p in range(1, local - 1):
        diagonal(p)
    middles.wait()
    bases.wait()
    for t in range(-local - 1, SWEEPS):
        outer_part(t)
        middle_part(t)
        offer_part(t)
        inner_part(t)
        after_part(t)

    for copy in (out_node, out_far, out_near, inners[0]):
        copy.wait_send()
    remote(held, pull, 0, 0, outer).wait_send()
    remote(u.at[:, local], u.at[:, local + 1], 1, 0, inner).wait_send()


def write_out(field, remain, rim_u, rim_m, out, rest, last, sem):
    local, _, nx, ny = field.shape
    odd = lax.rem(lax.axis_index("slab"), 2)
    sign = (1 - 2 * odd).astype(jnp.float32)
    copies = [pltpu.make_async_copy(field, out, sem.at[0])]
    for p in range(1, local):
        at = plane_of(odd, local, p)
        copies.append(pltpu.make_async_copy(remain.at[at], rest.at[at], sem.at[p]))
    for copy in copies:
        copy.start()
    at = plane_of(odd, local, 0)
    gx, gy, gz = zip(*(slopes(rim_u[c]) for c in range(3)))
    made = stresses(gx, gy, [-value for value in gz], rim_m[0], rim_m[1], rim_m[2])
    for c in range(3):
        x, y, z = STRESS[c]
        more = force(made[x], made[y], made[z])
        last[c] = remain[at, c] - (more * sign if c == 2 else more)
    copies.append(pltpu.make_async_copy(last, rest.at[at], sem.at[local]))
    copies[-1].start()
    for copy in copies:
        copy.wait()


def on_device(peers, displacement, load, phase, moduli):
    local, comps, nx, ny = displacement.shape
    plane = (nx, ny)
    hbm = pl.BlockSpec(memory_space=pl.ANY)
    f32 = jnp.float32
    vmem = pl.BlockSpec(memory_space=pltpu.VMEM)
    held = pl.pallas_call(
        functools.partial(kernel, peers),
        out_shape=[pltpu.VMEM(displacement.shape, f32)] * 2 + [pltpu.VMEM((comps,) + plane, f32)] * 2,
        in_specs=[hbm] * 4,
        out_specs=[vmem] * 4,
        scratch_shapes=[
            pltpu.SMEM(moduli.shape, f32),
            pltpu.VMEM((local + 2, comps) + plane, f32),
            pltpu.VMEM((SWEEPS, local + 2, comps) + plane, f32),
            pltpu.VMEM((local, comps) + plane, f32),
            pltpu.VMEM((local + 2,) + plane, jnp.int32),
            pltpu.VMEM((local + 2,) + plane, f32),
            pltpu.VMEM((local + 2,) + plane, f32),
            pltpu.VMEM((local + 2,) + plane, f32),
            pltpu.VMEM((local + 1,) + plane, f32),
            pltpu.VMEM((local + 2, 9) + plane, f32),
            pltpu.VMEM((local + 3, 6) + plane, f32),
            pltpu.VMEM((comps,) + plane, f32),
            pltpu.VMEM((SWEEPS, comps) + plane, f32),
            pltpu.VMEM((SWEEPS, comps) + plane, f32),
            pltpu.SemaphoreType.DMA((6,)),
            pltpu.SemaphoreType.DMA((6,)),
            pltpu.SemaphoreType.DMA((SWEEPS + 5,)),
        ],
        compiler_params=pltpu.CompilerParams(collective_id=0, has_side_effects=True),
    )(displacement, load, phase, moduli)
    return pl.pallas_call(
        write_out,
        out_shape=[jax.ShapeDtypeStruct(displacement.shape, f32)] * 2,
        in_specs=[vmem] * 4,
        out_specs=[hbm, hbm],
        scratch_shapes=[pltpu.VMEM((comps,) + plane, f32), pltpu.SemaphoreType.DMA((local + 1,))],
    )(*[pltpu.with_memory_space_constraint(one, pltpu.VMEM) for one in held])


def solution(mesh):
    in_specs = (
        P("slab", None, "rve", None),
        P("slab", None, "rve", None),
        P("slab", "rve", None),
        P(),
    )
    out_specs = (P("slab", None, "rve", None), P("slab", None, "rve", None))
    return jax.shard_map(
        functools.partial(on_device, mesh.shape["slab"]),
        mesh=mesh, in_specs=in_specs, out_specs=out_specs, check_vma=False,
    )
```

```python
import functools

import jax
import jax.numpy as jnp
from jax import lax
from jax.experimental import pallas as pl
from jax.experimental.pallas import tpu as pltpu
from jax.sharding import PartitionSpec as P

SWEEPS = 6
MESH = pl.DeviceIdType.MESH
ROWS = 8
LATE = range(SWEEPS // 2, SWEEPS)

STRESS = ((0, 3, 4), (3, 1, 5), (4, 5, 2))


def shift_next(value, axis):
    return pltpu.roll(value, value.shape[axis] - 1, axis)


def shift_prev(value, axis):
    return pltpu.roll(value, 1, axis)


def slopes(value):
    moved = shift_next(value, 1)
    total, jump = value + moved, moved - value
    moved = shift_next(total, 0)
    return moved - total, jump + shift_next(jump, 0), moved + total


def stresses(gx, gy, gz, lam, mu, mu2):
    bulk = lam * (gx[0] + gy[1] + gz[2])
    return (
        bulk + mu2 * gx[0], bulk + mu2 * gy[1], bulk + mu2 * gz[2],
        mu * (gy[0] + gx[1]), mu * (gz[0] + gx[2]), mu * (gz[1] + gy[2]),
    )


def force(px, qy, rz):
    e = (rz - px) + shift_prev(rz + px, 0)
    b = qy + shift_prev(qy, 0)
    return (e - b) + shift_prev(e + b, 1)


def plane_of(odd, local, p):
    return jnp.where(odd == 1, local - 1 - p, p)


def kernel(
    peers, disp, load, phase, table, out, rest, rim_u, rim_m,
    moduli, raw, u, ld, ph, lam, mu, mu2, inv, fwd, st, near, held, pull,
    in_sem, send_sem, recv_sem,
):
    local, _, nx, ny = disp.shape
    phases = table.shape[1]
    me = lax.axis_index("slab")
    odd = lax.rem(me, 2)
    closing = jnp.logical_or(me == 0, me == peers - 1)
    sign = (1 - 2 * odd).astype(jnp.float32)
    outer = lax.rem(me + 2 * odd - 1 + peers, peers)
    inner = me + 1 - 2 * odd

    def plane(p):
        return plane_of(odd, local, p)

    barrier = pltpu.get_barrier_semaphore()
    for peer in (outer, inner):
        pl.semaphore_signal(barrier, inc=1, device_id={"slab": peer}, device_id_type=MESH)

    def bring(src, dst, at):
        return pltpu.make_async_copy(src, dst, in_sem.at[at])

    def bring_node(p, at):
        return bring(disp.at[plane(p)], raw.at[p + 1], at)

    rim, hub, consts = bring_node(0, 0), bring_node(local - 1, 1), bring(table, moduli, 2)
    kinds = bring(phase, ph.at[pl.ds(2, local)], 3)
    middles = bring(disp.at[pl.ds(1, local - 2)], raw.at[pl.ds(2, local - 2)], 4)
    bases = bring(load, ld, 5)
    rim.start()
    hub.start()
    for k in range(local):
        bring(phase.at[k], ph.at[jnp.where(odd == 1, local - k, k + 2)], 3).start()
    consts.start()
    for p in range(1, local - 1):
        bring_node(p, 4).start()
    for p in range(local):
        bring(load.at[plane(p)], ld.at[p], 5).start()

    pl.semaphore_wait(barrier, 2)

    def remote(src, dst, send, recv, peer):
        return pltpu.make_async_remote_copy(
            src_ref=src, dst_ref=dst, send_sem=send_sem.at[send], recv_sem=recv_sem.at[recv],
            device_id={"slab": peer}, device_id_type=MESH,
        )

    out_node = remote(raw.at[1], raw.at[0], 2, SWEEPS, outer)
    out_far = remote(ph.at[2], ph.at[0], 3, SWEEPS + 1, outer)
    out_near = remote(ph.at[1], ph.at[1], 4, SWEEPS + 2, outer)
    in_kind = remote(ph.at[local + 1], ph.at[local + 1], 4, SWEEPS + 2, inner)
    pulls = [remote(held.at[s], pull.at[s], 0, s, outer) for s in range(SWEEPS)]

    def at_level(s, p):
        return raw.at[p + 1] if s == 0 else u.at[s - 1, p + 1]

    inners = [
        remote(at_level(s, local - 1), at_level(s, local), 1 if s else 5, SWEEPS + 3 + s % 2, inner)
        for s in range(SWEEPS + 1)
    ]

    rim.wait()
    out_node.start()
    hub.wait()
    inners[0].start()
    kinds.wait()

    @pl.when(odd == 1)
    def _():
        out_near.start()

    @pl.when(odd == 0)
    def _():
        in_kind.start()

    out_far.start()

    def value_at(s, p, c):
        value = at_level(s, p)[c]
        if c == 2 and s == 0:
            return value * sign
        if c == 2 and p == local:
            return -value
        return value

    def material(e):
        for r in range(0, nx, ROWS):
            at = pl.ds(r, ROWS)
            kind = ph[e + 2, at, :]
            lame = jnp.zeros(kind.shape, jnp.float32)
            shear = jnp.zeros(kind.shape, jnp.float32)
            for index in range(phases):
                lame = jnp.where(kind == index, moduli[0, index] * 0.0625, lame)
                shear = jnp.where(kind == index, moduli[1, index] * 0.0625, shear)
            lam[e + 2, at, :] = lame
            mu[e + 2, at, :] = shear
            mu2[e + 2, at, :] = shear + shear

    def diagonal(p):
        total = (lam[p + 1] + 2.0 * mu2[p + 1]) + (lam[p + 2] + 2.0 * mu2[p + 2])
        total = total + shift_prev(total, 1)
        total = total + shift_prev(total, 0)
        inv[p + 1] = 0.5 / total

    def forward(s, p):
        for c in range(3):
            x, y, z = slopes(value_at(s, p, c))
            fwd[p + 1, c], fwd[p + 1, 3 + c], fwd[p + 1, 6 + c] = x, y, z

    def element(e, half=False, into=None):
        lo, hi = e + 1, e + 2
        to = e + 2 if into is None else into
        for r in range(0, nx, ROWS):
            at = pl.ds(r, ROWS)
            gx, gy, gz = ([fwd[hi, 3 * a + c, at, :] for c in range(3)] for a in range(3))
            if not half:
                gx = [gx[c] + fwd[lo, c, at, :] for c in range(3)]
                gy = [gy[c] + fwd[lo, 3 + c, at, :] for c in range(3)]
                gz = [gz[c] - fwd[lo, 6 + c, at, :] for c in range(3)]
            made = stresses(gx, gy, gz, lam[e + 2, at, :], mu[e + 2, at, :], mu2[e + 2, at, :])
            for k in range(6):
                st[to, k, at, :] = made[k]

    def internal(p, c):
        lo, hi = p + 1, p + 2
        x, y, z = STRESS[c]
        return force(st[lo, x] + st[hi, x], st[lo, y] + st[hi, y], st[lo, z] - st[hi, z])

    def based(p, c):
        return ld[p, c] * sign if c == 2 else ld[p, c]

    def settle(s, p, c, value):
        if p < 0 and s == SWEEPS:
            rim_u[c] = value
            return
        u[s - 1, p + 1, c] = value
        if s == SWEEPS and 0 <= p < local:
            out[plane(p), c] = value * sign if c == 2 else value

    def advance(s, p):
        for c in range(3):
            remain = based(p, c) - internal(p, c)
            if s > SWEEPS:
                rest[plane(p), c] = remain * sign if c == 2 else remain
            else:
                settle(s, p, c, value_at(s - 1, p, c) + inv[p + 1] * remain)

    def prepare(s):
        element(-2, half=True)
        for c in range(3):
            near[c] = value_at(s - 1, -1, c) - inv[0] * internal(-1, c)

    def land(s):
        for c in range(3):
            drawn = inv[0] * pull[s - 1, c]
            settle(s, -1, c, near[c] - drawn if c == 2 else near[c] + drawn)

    spare = local + 2

    def offer(s):
        element(0, half=True, into=spare)
        for c in range(3):
            x, y, z = STRESS[c]
            held[s, c] = based(0, c) - force(st[spare, x], st[spare, y], -st[spare, z])
        if s not in LATE:
            pulls[s].start()
        else:
            pl.when(closing)(pulls[s].start)

    def leave():
        element(-1, half=True)
        for c in range(3):
            remain = based(0, c) - internal(0, c)
            rest[plane(0), c] = remain * sign if c == 2 else remain
        for k, field in enumerate((lam, mu, mu2)):
            rim_m[k] = field[1]

    def outer_part(t):
        if t == -1:
            out_node.wait_recv()

            @pl.when(odd == 0)
            def _():
                out_near.wait_recv()

            material(-1)
            diagonal(0)
        if 0 <= t < SWEEPS:
            pulls[t].wait_recv()
            land(t + 1)
        if -1 <= t < SWEEPS - 1:
            forward(t + 1, -1)
            element(-1)
            advance(t + 2, 0)
            if t + 2 in LATE[:-1]:
                pl.when(jnp.logical_not(closing))(pulls[t + 2].start)

    def middle_part(t):
        if 0 <= t + 2 <= SWEEPS:
            forward(t + 2, 0)
            element(0)
            advance(t + 3, 1)

    def offer_part(t):
        if 0 <= t + 3 <= SWEEPS:
            forward(t + 3, 1)
        if 0 <= t + 3 < SWEEPS:
            offer(t + 3)

    def inner_part(t):
        for p in range(2, local):
            if 0 <= t + p + 1 <= SWEEPS:
                if p > 2:
                    forward(t + p + 1, p - 1)
                element(p - 1)
                if p == local - 1:
                    inners[t + p + 1].wait_recv()
                    if t + p + 1 == 0:

                        @pl.when(odd == 1)
                        def _():
                            in_kind.wait_recv()

                        material(local - 1)
                        diagonal(local - 1)
                    forward(t + p + 1, local)
                    element(local - 1)
                advance(t + p + 2, p)
                if p == local - 1 and t + p + 2 <= SWEEPS:
                    inners[t + p + 2].start()
        if 0 <= t + local + 1 <= SWEEPS:
            forward(t + local + 1, local - 1)

    def after_part(t):
        if t == -1:
            out_far.wait_recv()
            material(-2)
            diagonal(-1)
        if -1 <= t < SWEEPS - 1:
            prepare(t + 2)
        if t == SWEEPS - 2:
            leave()
        if t + 2 == LATE[-1]:
            pl.when(jnp.logical_not(closing))(pulls[t + 2].start)

    consts.wait()
    for p in range(local - 1):
        material(p)
    for p in range(1, local - 1):
        diagonal(p)
    middles.wait()
    bases.wait()
    for t in range(-local - 1, SWEEPS):
        outer_part(t)
        middle_part(t)
        offer_part(t)
        inner_part(t)
        after_part(t)

    for copy in (out_node, out_far, out_near, inners[0]):
        copy.wait_send()
    remote(held, pull, 0, 0, outer).wait_send()
    remote(u.at[:, local], u.at[:, local + 1], 1, 0, inner).wait_send()


def write_out(field, remain, rim_u, rim_m, out, rest, last, sem):
    local, _, nx, ny = field.shape
    odd = lax.rem(lax.axis_index("slab"), 2)
    sign = (1 - 2 * odd).astype(jnp.float32)
    copies = [pltpu.make_async_copy(field, out, sem.at[0])]
    for p in range(1, local):
        at = plane_of(odd, local, p)
        copies.append(pltpu.make_async_copy(remain.at[at], rest.at[at], sem.at[p]))
    for copy in copies:
        copy.start()
    at = plane_of(odd, local, 0)
    gx, gy, gz = zip(*(slopes(rim_u[c]) for c in range(3)))
    made = stresses(gx, gy, [-value for value in gz], rim_m[0], rim_m[1], rim_m[2])
    for c in range(3):
        x, y, z = STRESS[c]
        more = force(made[x], made[y], made[z])
        last[c] = remain[at, c] - (more * sign if c == 2 else more)
    copies.append(pltpu.make_async_copy(last, rest.at[at], sem.at[local]))
    copies[-1].start()
    for copy in copies:
        copy.wait()


def on_device(peers, displacement, load, phase, moduli):
    local, comps, nx, ny = displacement.shape
    plane = (nx, ny)
    hbm = pl.BlockSpec(memory_space=pl.ANY)
    f32 = jnp.float32
    vmem = pl.BlockSpec(memory_space=pltpu.VMEM)
    held = pl.pallas_call(
        functools.partial(kernel, peers),
        out_shape=[pltpu.VMEM(displacement.shape, f32)] * 2 + [pltpu.VMEM((comps,) + plane, f32)] * 2,
        in_specs=[hbm] * 4,
        out_specs=[vmem] * 4,
        scratch_shapes=[
            pltpu.SMEM(moduli.shape, f32),
            pltpu.VMEM((local + 2, comps) + plane, f32),
            pltpu.VMEM((SWEEPS, local + 2, comps) + plane, f32),
            pltpu.VMEM((local, comps) + plane, f32),
            pltpu.VMEM((local + 2,) + plane, jnp.int32),
            pltpu.VMEM((local + 2,) + plane, f32),
            pltpu.VMEM((local + 2,) + plane, f32),
            pltpu.VMEM((local + 2,) + plane, f32),
            pltpu.VMEM((local + 1,) + plane, f32),
            pltpu.VMEM((local + 2, 9) + plane, f32),
            pltpu.VMEM((local + 3, 6) + plane, f32),
            pltpu.VMEM((comps,) + plane, f32),
            pltpu.VMEM((SWEEPS, comps) + plane, f32),
            pltpu.VMEM((SWEEPS, comps) + plane, f32),
            pltpu.SemaphoreType.DMA((6,)),
            pltpu.SemaphoreType.DMA((6,)),
            pltpu.SemaphoreType.DMA((SWEEPS + 5,)),
        ],
        compiler_params=pltpu.CompilerParams(collective_id=0, has_side_effects=True),
    )(displacement, load, phase, moduli)
    return pl.pallas_call(
        write_out,
        out_shape=[jax.ShapeDtypeStruct(displacement.shape, f32)] * 2,
        in_specs=[vmem] * 4,
        out_specs=[hbm, hbm],
        scratch_shapes=[pltpu.VMEM((comps,) + plane, f32), pltpu.SemaphoreType.DMA((local + 1,))],
    )(*[pltpu.with_memory_space_constraint(one, pltpu.VMEM) for one in held])


def solution(mesh):
    in_specs = (
        P("slab", None, "rve", None),
        P("slab", None, "rve", None),
        P("slab", "rve", None),
        P(),
    )
    out_specs = (P("slab", None, "rve", None), P("slab", None, "rve", None))
    return jax.shard_map(
        functools.partial(on_device, mesh.shape["slab"]),
        mesh=mesh, in_specs=in_specs, out_specs=out_specs, check_vma=False,
    )
```

```python
import functools

import jax
import jax.numpy as jnp
from jax import lax
from jax.experimental import pallas as pl
from jax.experimental.pallas import tpu as pltpu
from jax.sharding import PartitionSpec as P

SWEEPS = 6
MESH = pl.DeviceIdType.MESH
ROWS = 8
LATE = range(SWEEPS // 2, SWEEPS)

STRESS = ((0, 3, 4), (3, 1, 5), (4, 5, 2))


def shift_next(value, axis):
    return pltpu.roll(value, value.shape[axis] - 1, axis)


def shift_prev(value, axis):
    return pltpu.roll(value, 1, axis)


def slopes(value):
    moved = shift_next(value, 1)
    total, jump = value + moved, moved - value
    moved = shift_next(total, 0)
    return moved - total, jump + shift_next(jump, 0), moved + total


def stresses(gx, gy, gz, lam, mu, mu2):
    bulk = lam * (gx[0] + gy[1] + gz[2])
    return (
        bulk + mu2 * gx[0], bulk + mu2 * gy[1], bulk + mu2 * gz[2],
        mu * (gy[0] + gx[1]), mu * (gz[0] + gx[2]), mu * (gz[1] + gy[2]),
    )


def force(px, qy, rz):
    e = (rz - px) + shift_prev(rz + px, 0)
    b = qy + shift_prev(qy, 0)
    return (e - b) + shift_prev(e + b, 1)


def plane_of(odd, local, p):
    return jnp.where(odd == 1, local - 1 - p, p)


def kernel(
    peers, disp, load, phase, table, out, rest, rim_u, rim_m,
    moduli, raw, u, ld, ph, lam, mu, mu2, inv, fwd, st, near, held, pull,
    in_sem, send_sem, recv_sem,
):
    local, _, nx, ny = disp.shape
    phases = table.shape[1]
    me = lax.axis_index("slab")
    odd = lax.rem(me, 2)
    closing = jnp.logical_or(me == 0, me == peers - 1)
    patient = jnp.logical_and(odd == 0, me > 2)
    sign = (1 - 2 * odd).astype(jnp.float32)
    outer = lax.rem(me + 2 * odd - 1 + peers, peers)
    inner = me + 1 - 2 * odd

    def plane(p):
        return plane_of(odd, local, p)

    barrier = pltpu.get_barrier_semaphore()
    for peer in (outer, inner):
        pl.semaphore_signal(barrier, inc=1, device_id={"slab": peer}, device_id_type=MESH)

    def bring(src, dst, at):
        return pltpu.make_async_copy(src, dst, in_sem.at[at])

    def bring_node(p, at):
        return bring(disp.at[plane(p)], raw.at[p + 1], at)

    rim, hub, consts = bring_node(0, 0), bring_node(local - 1, 1), bring(table, moduli, 2)
    kinds = bring(phase, ph.at[pl.ds(2, local)], 3)
    middles = bring(disp.at[pl.ds(1, local - 2)], raw.at[pl.ds(2, local - 2)], 4)
    bases = bring(load, ld, 5)
    rim.start()
    hub.start()
    for k in range(local):
        bring(phase.at[k], ph.at[jnp.where(odd == 1, local - k, k + 2)], 3).start()
    consts.start()
    for p in range(1, local - 1):
        bring_node(p, 4).start()
    for p in range(local):
        bring(load.at[plane(p)], ld.at[p], 5).start()

    pl.semaphore_wait(barrier, 2)

    def remote(src, dst, send, recv, peer):
        return pltpu.make_async_remote_copy(
            src_ref=src, dst_ref=dst, send_sem=send_sem.at[send], recv_sem=recv_sem.at[recv],
            device_id={"slab": peer}, device_id_type=MESH,
        )

    out_node = remote(raw.at[1], raw.at[0], 2, SWEEPS, outer)
    out_far = remote(ph.at[2], ph.at[0], 3, SWEEPS + 1, outer)
    out_near = remote(ph.at[1], ph.at[1], 4, SWEEPS + 2, outer)
    in_kind = remote(ph.at[local + 1], ph.at[local + 1], 4, SWEEPS + 2, inner)
    pulls = [remote(held.at[s], pull.at[s], 0, s, outer) for s in range(SWEEPS)]

    def at_level(s, p):
        return raw.at[p + 1] if s == 0 else u.at[s - 1, p + 1]

    inners = [
        remote(at_level(s, local - 1), at_level(s, local), 1 if s else 5, SWEEPS + 3 + s % 2, inner)
        for s in range(SWEEPS + 1)
    ]

    rim.wait()
    out_node.start()
    hub.wait()
    inners[0].start()
    kinds.wait()

    @pl.when(odd == 1)
    def _():
        out_near.start()

    @pl.when(odd == 0)
    def _():
        in_kind.start()

    out_far.start()

    def value_at(s, p, c):
        value = at_level(s, p)[c]
        if c == 2 and s == 0:
            return value * sign
        if c == 2 and p == local:
            return -value
        return value

    def material(e):
        for r in range(0, nx, ROWS):
            at = pl.ds(r, ROWS)
            kind = ph[e + 2, at, :]
            lame = jnp.zeros(kind.shape, jnp.float32)
            shear = jnp.zeros(kind.shape, jnp.float32)
            for index in range(phases):
                lame = jnp.where(kind == index, moduli[0, index] * 0.0625, lame)
                shear = jnp.where(kind == index, moduli[1, index] * 0.0625, shear)
            lam[e + 2, at, :] = lame
            mu[e + 2, at, :] = shear
            mu2[e + 2, at, :] = shear + shear

    def diagonal(p):
        total = (lam[p + 1] + 2.0 * mu2[p + 1]) + (lam[p + 2] + 2.0 * mu2[p + 2])
        total = total + shift_prev(total, 1)
        total = total + shift_prev(total, 0)
        inv[p + 1] = 0.5 / total

    def forward(s, p):
        for c in range(3):
            x, y, z = slopes(value_at(s, p, c))
            fwd[p + 1, c], fwd[p + 1, 3 + c], fwd[p + 1, 6 + c] = x, y, z

    def element(e, half=False, into=None):
        lo, hi = e + 1, e + 2
        to = e + 2 if into is None else into
        for r in range(0, nx, ROWS):
            at = pl.ds(r, ROWS)
            gx, gy, gz = ([fwd[hi, 3 * a + c, at, :] for c in range(3)] for a in range(3))
            if not half:
                gx = [gx[c] + fwd[lo, c, at, :] for c in range(3)]
                gy = [gy[c] + fwd[lo, 3 + c, at, :] for c in range(3)]
                gz = [gz[c] - fwd[lo, 6 + c, at, :] for c in range(3)]
            made = stresses(gx, gy, gz, lam[e + 2, at, :], mu[e + 2, at, :], mu2[e + 2, at, :])
            for k in range(6):
                st[to, k, at, :] = made[k]

    def internal(p, c):
        lo, hi = p + 1, p + 2
        x, y, z = STRESS[c]
        return force(st[lo, x] + st[hi, x], st[lo, y] + st[hi, y], st[lo, z] - st[hi, z])

    def based(p, c):
        return ld[p, c] * sign if c == 2 else ld[p, c]

    def settle(s, p, c, value):
        if p < 0 and s == SWEEPS:
            rim_u[c] = value
            return
        u[s - 1, p + 1, c] = value
        if s == SWEEPS and 0 <= p < local:
            out[plane(p), c] = value * sign if c == 2 else value

    def advance(s, p):
        for c in range(3):
            remain = based(p, c) - internal(p, c)
            if s > SWEEPS:
                rest[plane(p), c] = remain * sign if c == 2 else remain
            else:
                settle(s, p, c, value_at(s - 1, p, c) + inv[p + 1] * remain)

    def prepare(s):
        element(-2, half=True)
        for c in range(3):
            near[c] = value_at(s - 1, -1, c) - inv[0] * internal(-1, c)

    def land(s):
        for c in range(3):
            drawn = inv[0] * pull[s - 1, c]
            settle(s, -1, c, near[c] - drawn if c == 2 else near[c] + drawn)

    spare = local + 2

    def offer(s):
        element(0, half=True, into=spare)
        for c in range(3):
            x, y, z = STRESS[c]
            held[s, c] = based(0, c) - force(st[spare, x], st[spare, y], -st[spare, z])
        if s not in LATE:
            pulls[s].start()
        else:
            pl.when(closing)(pulls[s].start)

    def leave():
        element(-1, half=True)
        for c in range(3):
            remain = based(0, c) - internal(0, c)
            rest[plane(0), c] = remain * sign if c == 2 else remain
        for k, field in enumerate((lam, mu, mu2)):
            rim_m[k] = field[1]

    def outer_part(t):
        if t == -1:
            out_node.wait_recv()

            @pl.when(odd == 0)
            def _():
                out_near.wait_recv()

            material(-1)
            diagonal(0)
        if 0 <= t < SWEEPS:
            pulls[t].wait_recv()
            land(t + 1)
        if -1 <= t < SWEEPS - 1:
            forward(t + 1, -1)
            element(-1)
            advance(t + 2, 0)
            if t + 2 in LATE[:-2]:
                pl.when(jnp.logical_not(closing))(pulls[t + 2].start)
            if t + 2 == LATE[-2]:
                pl.when(jnp.logical_not(jnp.logical_or(closing, patient)))(pulls[t + 2].start)

    def middle_part(t):
        if 0 <= t + 2 <= SWEEPS:
            forward(t + 2, 0)
            element(0)
            advance(t + 3, 1)

    def offer_part(t):
        if 0 <= t + 3 <= SWEEPS:
            forward(t + 3, 1)
        if 0 <= t + 3 < SWEEPS:
            offer(t + 3)

    def inner_part(t):
        for p in range(2, local):
            if 0 <= t + p + 1 <= SWEEPS:
                if p > 2:
                    forward(t + p + 1, p - 1)
                element(p - 1)
                if p == local - 1:
                    inners[t + p + 1].wait_recv()
                    if t + p + 1 == 0:

                        @pl.when(odd == 1)
                        def _():
                            in_kind.wait_recv()

                        material(local - 1)
                        diagonal(local - 1)
                    forward(t + p + 1, local)
                    element(local - 1)
                advance(t + p + 2, p)
                if p == local - 1 and t + p + 2 <= SWEEPS:
                    inners[t + p + 2].start()
        if 0 <= t + local + 1 <= SWEEPS:
            forward(t + local + 1, local - 1)

    def after_part(t):
        if t == -1:
            out_far.wait_recv()
            material(-2)
            diagonal(-1)
        if -1 <= t < SWEEPS - 1:
            prepare(t + 2)
        if t == SWEEPS - 2:
            leave()
        if t + 2 == LATE[-2]:
            pl.when(patient)(pulls[t + 2].start)
        if t + 2 == LATE[-1]:
            pl.when(jnp.logical_not(closing))(pulls[t + 2].start)

    consts.wait()
    for p in range(local - 1):
        material(p)
    for p in range(1, local - 1):
        diagonal(p)
    middles.wait()
    bases.wait()
    for t in range(-local - 1, SWEEPS):
        outer_part(t)
        middle_part(t)
        offer_part(t)
        inner_part(t)
        after_part(t)

    for copy in (out_node, out_far, out_near, inners[0]):
        copy.wait_send()
    remote(held, pull, 0, 0, outer).wait_send()
    remote(u.at[:, local], u.at[:, local + 1], 1, 0, inner).wait_send()


def write_out(field, remain, rim_u, rim_m, out, rest, last, sem):
    local, _, nx, ny = field.shape
    odd = lax.rem(lax.axis_index("slab"), 2)
    sign = (1 - 2 * odd).astype(jnp.float32)
    copies = [pltpu.make_async_copy(field, out, sem.at[0])]
    for p in range(1, local):
        at = plane_of(odd, local, p)
        copies.append(pltpu.make_async_copy(remain.at[at], rest.at[at], sem.at[p]))
    for copy in copies:
        copy.start()
    at = plane_of(odd, local, 0)
    gx, gy, gz = zip(*(slopes(rim_u[c]) for c in range(3)))
    made = stresses(gx, gy, [-value for value in gz], rim_m[0], rim_m[1], rim_m[2])
    for c in range(3):
        x, y, z = STRESS[c]
        more = force(made[x], made[y], made[z])
        last[c] = remain[at, c] - (more * sign if c == 2 else more)
    copies.append(pltpu.make_async_copy(last, rest.at[at], sem.at[local]))
    copies[-1].start()
    for copy in copies:
        copy.wait()


def on_device(peers, displacement, load, phase, moduli):
    local, comps, nx, ny = displacement.shape
    plane = (nx, ny)
    hbm = pl.BlockSpec(memory_space=pl.ANY)
    f32 = jnp.float32
    vmem = pl.BlockSpec(memory_space=pltpu.VMEM)
    held = pl.pallas_call(
        functools.partial(kernel, peers),
        out_shape=[pltpu.VMEM(displacement.shape, f32)] * 2 + [pltpu.VMEM((comps,) + plane, f32)] * 2,
        in_specs=[hbm] * 4,
        out_specs=[vmem] * 4,
        scratch_shapes=[
            pltpu.SMEM(moduli.shape, f32),
            pltpu.VMEM((local + 2, comps) + plane, f32),
            pltpu.VMEM((SWEEPS, local + 2, comps) + plane, f32),
            pltpu.VMEM((local, comps) + plane, f32),
            pltpu.VMEM((local + 2,) + plane, jnp.int32),
            pltpu.VMEM((local + 2,) + plane, f32),
            pltpu.VMEM((local + 2,) + plane, f32),
            pltpu.VMEM((local + 2,) + plane, f32),
            pltpu.VMEM((local + 1,) + plane, f32),
            pltpu.VMEM((local + 2, 9) + plane, f32),
            pltpu.VMEM((local + 3, 6) + plane, f32),
            pltpu.VMEM((comps,) + plane, f32),
            pltpu.VMEM((SWEEPS, comps) + plane, f32),
            pltpu.VMEM((SWEEPS, comps) + plane, f32),
            pltpu.SemaphoreType.DMA((6,)),
            pltpu.SemaphoreType.DMA((6,)),
            pltpu.SemaphoreType.DMA((SWEEPS + 5,)),
        ],
        compiler_params=pltpu.CompilerParams(collective_id=0, has_side_effects=True),
    )(displacement, load, phase, moduli)
    return pl.pallas_call(
        write_out,
        out_shape=[jax.ShapeDtypeStruct(displacement.shape, f32)] * 2,
        in_specs=[vmem] * 4,
        out_specs=[hbm, hbm],
        scratch_shapes=[pltpu.VMEM((comps,) + plane, f32), pltpu.SemaphoreType.DMA((local + 1,))],
    )(*[pltpu.with_memory_space_constraint(one, pltpu.VMEM) for one in held])


def solution(mesh):
    in_specs = (
        P("slab", None, "rve", None),
        P("slab", None, "rve", None),
        P("slab", "rve", None),
        P(),
    )
    out_specs = (P("slab", None, "rve", None), P("slab", None, "rve", None))
    return jax.shard_map(
        functools.partial(on_device, mesh.shape["slab"]),
        mesh=mesh, in_specs=in_specs, out_specs=out_specs, check_vma=False,
    )
```

```python
import functools

import jax
import jax.numpy as jnp
from jax import lax
from jax.experimental import pallas as pl
from jax.experimental.pallas import tpu as pltpu
from jax.sharding import PartitionSpec as P

SWEEPS = 6
MESH = pl.DeviceIdType.MESH
ROWS = 8
LATE = range(SWEEPS // 2, SWEEPS)

STRESS = ((0, 3, 4), (3, 1, 5), (4, 5, 2))


def shift_next(value, axis):
    return pltpu.roll(value, value.shape[axis] - 1, axis)


def shift_prev(value, axis):
    return pltpu.roll(value, 1, axis)


def slopes(value):
    moved = shift_next(value, 1)
    total, jump = value + moved, moved - value
    moved = shift_next(total, 0)
    return moved - total, jump + shift_next(jump, 0), moved + total


def stresses(gx, gy, gz, lam, mu, mu2):
    bulk = lam * (gx[0] + gy[1] + gz[2])
    return (
        bulk + mu2 * gx[0], bulk + mu2 * gy[1], bulk + mu2 * gz[2],
        mu * (gy[0] + gx[1]), mu * (gz[0] + gx[2]), mu * (gz[1] + gy[2]),
    )


def force(px, qy, rz):
    e = (rz - px) + shift_prev(rz + px, 0)
    b = qy + shift_prev(qy, 0)
    return (e - b) + shift_prev(e + b, 1)


def plane_of(odd, local, p):
    return jnp.where(odd == 1, local - 1 - p, p)


def kernel(
    peers, disp, load, phase, table, out, rest, rim_u, rim_m,
    moduli, raw, u, ld, ph, lam, mu, mu2, inv, fwd, st, near, held, pull,
    in_sem, send_sem, recv_sem,
):
    local, _, nx, ny = disp.shape
    phases = table.shape[1]
    me = lax.axis_index("slab")
    odd = lax.rem(me, 2)
    patient = jnp.logical_and(odd == 0, me > 2)
    sign = (1 - 2 * odd).astype(jnp.float32)
    outer = lax.rem(me + 2 * odd - 1 + peers, peers)
    inner = me + 1 - 2 * odd

    def plane(p):
        return plane_of(odd, local, p)

    barrier = pltpu.get_barrier_semaphore()
    for peer in (outer, inner):
        pl.semaphore_signal(barrier, inc=1, device_id={"slab": peer}, device_id_type=MESH)

    def bring(src, dst, at):
        return pltpu.make_async_copy(src, dst, in_sem.at[at])

    def bring_node(p, at):
        return bring(disp.at[plane(p)], raw.at[p + 1], at)

    rim, hub, consts = bring_node(0, 0), bring_node(local - 1, 1), bring(table, moduli, 2)
    kinds = bring(phase, ph.at[pl.ds(2, local)], 3)
    middles = bring(disp.at[pl.ds(1, local - 2)], raw.at[pl.ds(2, local - 2)], 4)
    bases = bring(load, ld, 5)
    rim.start()
    hub.start()
    for k in range(local):
        bring(phase.at[k], ph.at[jnp.where(odd == 1, local - k, k + 2)], 3).start()
    consts.start()
    for p in range(1, local - 1):
        bring_node(p, 4).start()
    for p in range(local):
        bring(load.at[plane(p)], ld.at[p], 5).start()

    pl.semaphore_wait(barrier, 2)

    def remote(src, dst, send, recv, peer):
        return pltpu.make_async_remote_copy(
            src_ref=src, dst_ref=dst, send_sem=send_sem.at[send], recv_sem=recv_sem.at[recv],
            device_id={"slab": peer}, device_id_type=MESH,
        )

    out_node = remote(raw.at[1], raw.at[0], 2, SWEEPS, outer)
    out_far = remote(ph.at[2], ph.at[0], 3, SWEEPS + 1, outer)
    out_near = remote(ph.at[1], ph.at[1], 4, SWEEPS + 2, outer)
    in_kind = remote(ph.at[local + 1], ph.at[local + 1], 4, SWEEPS + 2, inner)
    pulls = [remote(held.at[s], pull.at[s], 0, s, outer) for s in range(SWEEPS)]

    def at_level(s, p):
        return raw.at[p + 1] if s == 0 else u.at[s - 1, p + 1]

    inners = [
        remote(at_level(s, local - 1), at_level(s, local), 1 if s else 5, SWEEPS + 3 + s % 2, inner)
        for s in range(SWEEPS + 1)
    ]

    rim.wait()
    out_node.start()
    hub.wait()
    inners[0].start()
    kinds.wait()

    @pl.when(odd == 1)
    def _():
        out_near.start()

    @pl.when(odd == 0)
    def _():
        in_kind.start()

    out_far.start()

    def value_at(s, p, c):
        value = at_level(s, p)[c]
        if c == 2 and s == 0:
            return value * sign
        if c == 2 and p == local:
            return -value
        return value

    def material(e):
        for r in range(0, nx, ROWS):
            at = pl.ds(r, ROWS)
            kind = ph[e + 2, at, :]
            lame = jnp.zeros(kind.shape, jnp.float32)
            shear = jnp.zeros(kind.shape, jnp.float32)
            for index in range(phases):
                lame = jnp.where(kind == index, moduli[0, index] * 0.0625, lame)
                shear = jnp.where(kind == index, moduli[1, index] * 0.0625, shear)
            lam[e + 2, at, :] = lame
            mu[e + 2, at, :] = shear
            mu2[e + 2, at, :] = shear + shear

    def diagonal(p):
        total = (lam[p + 1] + 2.0 * mu2[p + 1]) + (lam[p + 2] + 2.0 * mu2[p + 2])
        total = total + shift_prev(total, 1)
        total = total + shift_prev(total, 0)
        inv[p + 1] = 0.5 / total

    def forward(s, p):
        for c in range(3):
            x, y, z = slopes(value_at(s, p, c))
            fwd[p + 1, c], fwd[p + 1, 3 + c], fwd[p + 1, 6 + c] = x, y, z

    def element(e, half=False, into=None):
        lo, hi = e + 1, e + 2
        to = e + 2 if into is None else into
        for r in range(0, nx, ROWS):
            at = pl.ds(r, ROWS)
            gx, gy, gz = ([fwd[hi, 3 * a + c, at, :] for c in range(3)] for a in range(3))
            if not half:
                gx = [gx[c] + fwd[lo, c, at, :] for c in range(3)]
                gy = [gy[c] + fwd[lo, 3 + c, at, :] for c in range(3)]
                gz = [gz[c] - fwd[lo, 6 + c, at, :] for c in range(3)]
            made = stresses(gx, gy, gz, lam[e + 2, at, :], mu[e + 2, at, :], mu2[e + 2, at, :])
            for k in range(6):
                st[to, k, at, :] = made[k]

    def internal(p, c):
        lo, hi = p + 1, p + 2
        x, y, z = STRESS[c]
        return force(st[lo, x] + st[hi, x], st[lo, y] + st[hi, y], st[lo, z] - st[hi, z])

    def based(p, c):
        return ld[p, c] * sign if c == 2 else ld[p, c]

    def settle(s, p, c, value):
        if p < 0 and s == SWEEPS:
            rim_u[c] = value
            return
        u[s - 1, p + 1, c] = value
        if s == SWEEPS and 0 <= p < local:
            out[plane(p), c] = value * sign if c == 2 else value

    def advance(s, p):
        for c in range(3):
            remain = based(p, c) - internal(p, c)
            if s > SWEEPS:
                rest[plane(p), c] = remain * sign if c == 2 else remain
            else:
                settle(s, p, c, value_at(s - 1, p, c) + inv[p + 1] * remain)

    def prepare(s):
        element(-2, half=True)
        for c in range(3):
            near[c] = value_at(s - 1, -1, c) - inv[0] * internal(-1, c)

    def land(s):
        for c in range(3):
            drawn = inv[0] * pull[s - 1, c]
            settle(s, -1, c, near[c] - drawn if c == 2 else near[c] + drawn)

    spare = local + 2

    def offer(s):
        element(0, half=True, into=spare)
        for c in range(3):
            x, y, z = STRESS[c]
            held[s, c] = based(0, c) - force(st[spare, x], st[spare, y], -st[spare, z])
        if s not in LATE:
            pulls[s].start()
        else:
            pl.when(jnp.logical_not(patient))(pulls[s].start)

    def leave():
        element(-1, half=True)
        for c in range(3):
            remain = based(0, c) - internal(0, c)
            rest[plane(0), c] = remain * sign if c == 2 else remain
        for k, field in enumerate((lam, mu, mu2)):
            rim_m[k] = field[1]

    def outer_part(t):
        if t == -1:
            out_node.wait_recv()

            @pl.when(odd == 0)
            def _():
                out_near.wait_recv()

            material(-1)
            diagonal(0)
        if 0 <= t < SWEEPS:
            pulls[t].wait_recv()
            land(t + 1)
        if -1 <= t < SWEEPS - 1:
            forward(t + 1, -1)
            element(-1)
            advance(t + 2, 0)
            if t + 2 in LATE[:-2]:
                pl.when(patient)(pulls[t + 2].start)

    def middle_part(t):
        if 0 <= t + 2 <= SWEEPS:
            forward(t + 2, 0)
            element(0)
            advance(t + 3, 1)

    def offer_part(t):
        if 0 <= t + 3 <= SWEEPS:
            forward(t + 3, 1)
        if 0 <= t + 3 < SWEEPS:
            offer(t + 3)

    def inner_part(t):
        for p in range(2, local):
            if 0 <= t + p + 1 <= SWEEPS:
                if p > 2:
                    forward(t + p + 1, p - 1)
                element(p - 1)
                if p == local - 1:
                    inners[t + p + 1].wait_recv()
                    if t + p + 1 == 0:

                        @pl.when(odd == 1)
                        def _():
                            in_kind.wait_recv()

                        material(local - 1)
                        diagonal(local - 1)
                    forward(t + p + 1, local)
                    element(local - 1)
                advance(t + p + 2, p)
                if p == local - 1 and t + p + 2 <= SWEEPS:
                    inners[t + p + 2].start()
        if 0 <= t + local + 1 <= SWEEPS:
            forward(t + local + 1, local - 1)

    def after_part(t):
        if t == -1:
            out_far.wait_recv()
            material(-2)
            diagonal(-1)
        if -1 <= t < SWEEPS - 1:
            prepare(t + 2)
        if t == SWEEPS - 2:
            leave()
        if t + 2 in LATE[-2:]:
            pl.when(patient)(pulls[t + 2].start)

    consts.wait()
    for p in range(local - 1):
        material(p)
    for p in range(1, local - 1):
        diagonal(p)
    middles.wait()
    bases.wait()
    for t in range(-local - 1, SWEEPS):
        outer_part(t)
        middle_part(t)
        offer_part(t)
        inner_part(t)
        after_part(t)

    for copy in (out_node, out_far, out_near, inners[0]):
        copy.wait_send()
    remote(held, pull, 0, 0, outer).wait_send()
    remote(u.at[:, local], u.at[:, local + 1], 1, 0, inner).wait_send()


def write_out(field, remain, rim_u, rim_m, out, rest, last, sem):
    local, _, nx, ny = field.shape
    odd = lax.rem(lax.axis_index("slab"), 2)
    sign = (1 - 2 * odd).astype(jnp.float32)
    copies = [pltpu.make_async_copy(field, out, sem.at[0])]
    for p in range(1, local):
        at = plane_of(odd, local, p)
        copies.append(pltpu.make_async_copy(remain.at[at], rest.at[at], sem.at[p]))
    for copy in copies:
        copy.start()
    at = plane_of(odd, local, 0)
    gx, gy, gz = zip(*(slopes(rim_u[c]) for c in range(3)))
    made = stresses(gx, gy, [-value for value in gz], rim_m[0], rim_m[1], rim_m[2])
    for c in range(3):
        x, y, z = STRESS[c]
        more = force(made[x], made[y], made[z])
        last[c] = remain[at, c] - (more * sign if c == 2 else more)
    copies.append(pltpu.make_async_copy(last, rest.at[at], sem.at[local]))
    copies[-1].start()
    for copy in copies:
        copy.wait()


def on_device(peers, displacement, load, phase, moduli):
    local, comps, nx, ny = displacement.shape
    plane = (nx, ny)
    hbm = pl.BlockSpec(memory_space=pl.ANY)
    f32 = jnp.float32
    vmem = pl.BlockSpec(memory_space=pltpu.VMEM)
    held = pl.pallas_call(
        functools.partial(kernel, peers),
        out_shape=[pltpu.VMEM(displacement.shape, f32)] * 2 + [pltpu.VMEM((comps,) + plane, f32)] * 2,
        in_specs=[hbm] * 4,
        out_specs=[vmem] * 4,
        scratch_shapes=[
            pltpu.SMEM(moduli.shape, f32),
            pltpu.VMEM((local + 2, comps) + plane, f32),
            pltpu.VMEM((SWEEPS, local + 2, comps) + plane, f32),
            pltpu.VMEM((local, comps) + plane, f32),
            pltpu.VMEM((local + 2,) + plane, jnp.int32),
            pltpu.VMEM((local + 2,) + plane, f32),
            pltpu.VMEM((local + 2,) + plane, f32),
            pltpu.VMEM((local + 2,) + plane, f32),
            pltpu.VMEM((local + 1,) + plane, f32),
            pltpu.VMEM((local + 2, 9) + plane, f32),
            pltpu.VMEM((local + 3, 6) + plane, f32),
            pltpu.VMEM((comps,) + plane, f32),
            pltpu.VMEM((SWEEPS, comps) + plane, f32),
            pltpu.VMEM((SWEEPS, comps) + plane, f32),
            pltpu.SemaphoreType.DMA((6,)),
            pltpu.SemaphoreType.DMA((6,)),
            pltpu.SemaphoreType.DMA((SWEEPS + 5,)),
        ],
        compiler_params=pltpu.CompilerParams(collective_id=0, has_side_effects=True),
    )(displacement, load, phase, moduli)
    return pl.pallas_call(
        write_out,
        out_shape=[jax.ShapeDtypeStruct(displacement.shape, f32)] * 2,
        in_specs=[vmem] * 4,
        out_specs=[hbm, hbm],
        scratch_shapes=[pltpu.VMEM((comps,) + plane, f32), pltpu.SemaphoreType.DMA((local + 1,))],
    )(*[pltpu.with_memory_space_constraint(one, pltpu.VMEM) for one in held])


def solution(mesh):
    in_specs = (
        P("slab", None, "rve", None),
        P("slab", None, "rve", None),
        P("slab", "rve", None),
        P(),
    )
    out_specs = (P("slab", None, "rve", None), P("slab", None, "rve", None))
    return jax.shard_map(
        functools.partial(on_device, mesh.shape["slab"]),
        mesh=mesh, in_specs=in_specs, out_specs=out_specs, check_vma=False,
    )
```

```python
import functools

import jax
import jax.numpy as jnp
from jax import lax
from jax.experimental import pallas as pl
from jax.experimental.pallas import tpu as pltpu
from jax.sharding import PartitionSpec as P

SWEEPS = 6
MESH = pl.DeviceIdType.MESH
ROWS = 8
LATE = range(SWEEPS // 2, SWEEPS)

STRESS = ((0, 3, 4), (3, 1, 5), (4, 5, 2))


def shift_next(value, axis):
    return pltpu.roll(value, value.shape[axis] - 1, axis)


def shift_prev(value, axis):
    return pltpu.roll(value, 1, axis)


def slopes(value):
    moved = shift_next(value, 1)
    total, jump = value + moved, moved - value
    moved = shift_next(total, 0)
    return moved - total, jump + shift_next(jump, 0), moved + total


def stresses(gx, gy, gz, lam, mu, mu2):
    bulk = lam * (gx[0] + gy[1] + gz[2])
    return (
        bulk + mu2 * gx[0], bulk + mu2 * gy[1], bulk + mu2 * gz[2],
        mu * (gy[0] + gx[1]), mu * (gz[0] + gx[2]), mu * (gz[1] + gy[2]),
    )


def force(px, qy, rz):
    e = (rz - px) + shift_prev(rz + px, 0)
    b = qy + shift_prev(qy, 0)
    return (e - b) + shift_prev(e + b, 1)


def plane_of(odd, local, p):
    return jnp.where(odd == 1, local - 1 - p, p)


def kernel(
    peers, disp, load, phase, table, out, rest, rim_u, rim_m,
    moduli, raw, u, ld, ph, lam, mu, mu2, inv, fwd, st, near, held, pull,
    in_sem, send_sem, recv_sem,
):
    local, _, nx, ny = disp.shape
    phases = table.shape[1]
    me = lax.axis_index("slab")
    odd = lax.rem(me, 2)
    patient = jnp.logical_and(odd == 0, me > 2)
    sign = (1 - 2 * odd).astype(jnp.float32)
    outer = lax.rem(me + 2 * odd - 1 + peers, peers)
    inner = me + 1 - 2 * odd

    def plane(p):
        return plane_of(odd, local, p)

    barrier = pltpu.get_barrier_semaphore()
    for peer in (outer, inner):
        pl.semaphore_signal(barrier, inc=1, device_id={"slab": peer}, device_id_type=MESH)

    def bring(src, dst, at):
        return pltpu.make_async_copy(src, dst, in_sem.at[at])

    def bring_node(p, at):
        return bring(disp.at[plane(p)], raw.at[p + 1], at)

    rim, hub, consts = bring_node(0, 0), bring_node(local - 1, 1), bring(table, moduli, 2)
    wide = u.at[pl.ds(0, 2), pl.ds(0, local - 1)]
    rests = bring(wide, wide, 3)
    early = bring(fwd.at[0, pl.ds(0, 3 + local)], fwd.at[1, pl.ds(0, 3 + local)], 1)
    rim.start()
    hub.start()
    for k in range(local):
        bring(phase.at[k], ph.at[jnp.where(odd == 1, local - k, k + 2)], 1).start()
    consts.start()
    for p in range(1, local - 1):
        bring_node(p, 3).start()
    for p in range(local):
        bring(load.at[plane(p)], ld.at[p], 3).start()

    pl.semaphore_wait(barrier, 2)

    def remote(src, dst, send, recv, peer):
        return pltpu.make_async_remote_copy(
            src_ref=src, dst_ref=dst, send_sem=send_sem.at[send], recv_sem=recv_sem.at[recv],
            device_id={"slab": peer}, device_id_type=MESH,
        )

    out_node = remote(raw.at[1], raw.at[0], 1, SWEEPS, outer)
    out_far = remote(ph.at[2], ph.at[0], 1, SWEEPS + 1, outer)
    out_near = remote(ph.at[1], ph.at[1], 1, SWEEPS + 2, outer)
    in_kind = remote(ph.at[local + 1], ph.at[local + 1], 1, SWEEPS + 2, inner)
    pulls = [remote(held.at[s], pull.at[s], 0, s, outer) for s in range(SWEEPS)]

    def at_level(s, p):
        return raw.at[p + 1] if s == 0 else u.at[s - 1, p + 1]

    inners = [
        remote(at_level(s, local - 1), at_level(s, local), 0 if s else 1, SWEEPS + 3 + s % 2, inner)
        for s in range(SWEEPS + 1)
    ]

    rim.wait()
    out_node.start()
    early.wait()
    inners[0].start()

    @pl.when(odd == 1)
    def _():
        out_near.start()

    @pl.when(odd == 0)
    def _():
        in_kind.start()

    out_far.start()

    def value_at(s, p, c):
        value = at_level(s, p)[c]
        if c == 2 and s == 0:
            return value * sign
        if c == 2 and p == local:
            return -value
        return value

    def material(e):
        for r in range(0, nx, ROWS):
            at = pl.ds(r, ROWS)
            kind = ph[e + 2, at, :]
            lame = jnp.zeros(kind.shape, jnp.float32)
            shear = jnp.zeros(kind.shape, jnp.float32)
            for index in range(phases):
                lame = jnp.where(kind == index, moduli[0, index] * 0.0625, lame)
                shear = jnp.where(kind == index, moduli[1, index] * 0.0625, shear)
            lam[e + 2, at, :] = lame
            mu[e + 2, at, :] = shear
            mu2[e + 2, at, :] = shear + shear

    def diagonal(p):
        total = (lam[p + 1] + 2.0 * mu2[p + 1]) + (lam[p + 2] + 2.0 * mu2[p + 2])
        total = total + shift_prev(total, 1)
        total = total + shift_prev(total, 0)
        inv[p + 1] = 0.5 / total

    def forward(s, p):
        for c in range(3):
            x, y, z = slopes(value_at(s, p, c))
            fwd[p + 1, c], fwd[p + 1, 3 + c], fwd[p + 1, 6 + c] = x, y, z

    def element(e, half=False, into=None):
        lo, hi = e + 1, e + 2
        to = e + 2 if into is None else into
        for r in range(0, nx, ROWS):
            at = pl.ds(r, ROWS)
            gx, gy, gz = ([fwd[hi, 3 * a + c, at, :] for c in range(3)] for a in range(3))
            if not half:
                gx = [gx[c] + fwd[lo, c, at, :] for c in range(3)]
                gy = [gy[c] + fwd[lo, 3 + c, at, :] for c in range(3)]
                gz = [gz[c] - fwd[lo, 6 + c, at, :] for c in range(3)]
            made = stresses(gx, gy, gz, lam[e + 2, at, :], mu[e + 2, at, :], mu2[e + 2, at, :])
            for k in range(6):
                st[to, k, at, :] = made[k]

    def internal(p, c):
        lo, hi = p + 1, p + 2
        x, y, z = STRESS[c]
        return force(st[lo, x] + st[hi, x], st[lo, y] + st[hi, y], st[lo, z] - st[hi, z])

    def based(p, c):
        return ld[p, c] * sign if c == 2 else ld[p, c]

    def settle(s, p, c, value):
        if p < 0 and s == SWEEPS:
            rim_u[c] = value
            return
        u[s - 1, p + 1, c] = value
        if s == SWEEPS and 0 <= p < local:
            out[plane(p), c] = value * sign if c == 2 else value

    def advance(s, p):
        for c in range(3):
            remain = based(p, c) - internal(p, c)
            if s > SWEEPS:
                rest[plane(p), c] = remain * sign if c == 2 else remain
            else:
                settle(s, p, c, value_at(s - 1, p, c) + inv[p + 1] * remain)

    def prepare(s):
        element(-2, half=True)
        for c in range(3):
            near[c] = value_at(s - 1, -1, c) - inv[0] * internal(-1, c)

    def land(s):
        for c in range(3):
            drawn = inv[0] * pull[s - 1, c]
            settle(s, -1, c, near[c] - drawn if c == 2 else near[c] + drawn)

    spare = local + 2

    def offer(s):
        element(0, half=True, into=spare)
        for c in range(3):
            x, y, z = STRESS[c]
            held[s, c] = based(0, c) - force(st[spare, x], st[spare, y], -st[spare, z])
        if s not in LATE:
            pulls[s].start()
        else:
            pl.when(jnp.logical_not(patient))(pulls[s].start)

    def leave():
        element(-1, half=True)
        for c in range(3):
            remain = based(0, c) - internal(0, c)
            rest[plane(0), c] = remain * sign if c == 2 else remain
        for k, field in enumerate((lam, mu, mu2)):
            rim_m[k] = field[1]

    def outer_part(t):
        if t == -1:
            out_node.wait_recv()

            @pl.when(odd == 0)
            def _():
                out_near.wait_recv()

            material(-1)
            diagonal(0)
        if 0 <= t < SWEEPS:
            pulls[t].wait_recv()
            land(t + 1)
        if -1 <= t < SWEEPS - 1:
            forward(t + 1, -1)
            element(-1)
            advance(t + 2, 0)
            if t + 2 in LATE[:-2]:
                pl.when(patient)(pulls[t + 2].start)

    def middle_part(t):
        if 0 <= t + 2 <= SWEEPS:
            forward(t + 2, 0)
            element(0)
            advance(t + 3, 1)

    def offer_part(t):
        if 0 <= t + 3 <= SWEEPS:
            forward(t + 3, 1)
        if 0 <= t + 3 < SWEEPS:
            offer(t + 3)

    def inner_part(t):
        for p in range(2, local):
            if 0 <= t + p + 1 <= SWEEPS:
                if p > 2:
                    forward(t + p + 1, p - 1)
                element(p - 1)
                if p == local - 1:
                    inners[t + p + 1].wait_recv()
                    if t + p + 1 == 0:

                        @pl.when(odd == 1)
                        def _():
                            in_kind.wait_recv()

                        material(local - 1)
                        diagonal(local - 1)
                    forward(t + p + 1, local)
                    element(local - 1)
                advance(t + p + 2, p)
                if p == local - 1 and t + p + 2 <= SWEEPS:
                    inners[t + p + 2].start()
        if 0 <= t + local + 1 <= SWEEPS:
            forward(t + local + 1, local - 1)

    def after_part(t):
        if t == -1:
            out_far.wait_recv()
            material(-2)
            diagonal(-1)
        if -1 <= t < SWEEPS - 1:
            prepare(t + 2)
        if t == SWEEPS - 2:
            leave()
        if t + 2 in LATE[-2:]:
            pl.when(patient)(pulls[t + 2].start)

    consts.wait()
    for p in range(local - 1):
        material(p)
    for p in range(1, local - 1):
        diagonal(p)
    rests.wait()
    for t in range(-local - 1, SWEEPS):
        outer_part(t)
        middle_part(t)
        offer_part(t)
        inner_part(t)
        after_part(t)

    remote(fwd.at[0, pl.ds(0, 8)], fwd.at[1, pl.ds(0, 8)], 1, 0, outer).wait_send()
    remote(u.at[:, pl.ds(0, 2)], u.at[:, pl.ds(0, 2)], 0, 0, outer).wait_send()


def write_out(field, remain, rim_u, rim_m, out, rest, last, sem):
    local, _, nx, ny = field.shape
    odd = lax.rem(lax.axis_index("slab"), 2)
    sign = (1 - 2 * odd).astype(jnp.float32)
    copies = [pltpu.make_async_copy(field, out, sem.at[0])]
    for p in range(1, local):
        at = plane_of(odd, local, p)
        copies.append(pltpu.make_async_copy(remain.at[at], rest.at[at], sem.at[p]))
    for copy in copies:
        copy.start()
    at = plane_of(odd, local, 0)
    gx, gy, gz = zip(*(slopes(rim_u[c]) for c in range(3)))
    made = stresses(gx, gy, [-value for value in gz], rim_m[0], rim_m[1], rim_m[2])
    for c in range(3):
        x, y, z = STRESS[c]
        more = force(made[x], made[y], made[z])
        last[c] = remain[at, c] - (more * sign if c == 2 else more)
    copies.append(pltpu.make_async_copy(last, rest.at[at], sem.at[local]))
    copies[-1].start()
    for copy in copies:
        copy.wait()


def on_device(peers, displacement, load, phase, moduli):
    local, comps, nx, ny = displacement.shape
    plane = (nx, ny)
    hbm = pl.BlockSpec(memory_space=pl.ANY)
    f32 = jnp.float32
    vmem = pl.BlockSpec(memory_space=pltpu.VMEM)
    held = pl.pallas_call(
        functools.partial(kernel, peers),
        out_shape=[pltpu.VMEM(displacement.shape, f32)] * 2 + [pltpu.VMEM((comps,) + plane, f32)] * 2,
        in_specs=[hbm] * 4,
        out_specs=[vmem] * 4,
        scratch_shapes=[
            pltpu.SMEM(moduli.shape, f32),
            pltpu.VMEM((local + 2, comps) + plane, f32),
            pltpu.VMEM((SWEEPS, local + 2, comps) + plane, f32),
            pltpu.VMEM((local, comps) + plane, f32),
            pltpu.VMEM((local + 2,) + plane, jnp.int32),
            pltpu.VMEM((local + 2,) + plane, f32),
            pltpu.VMEM((local + 2,) + plane, f32),
            pltpu.VMEM((local + 2,) + plane, f32),
            pltpu.VMEM((local + 1,) + plane, f32),
            pltpu.VMEM((local + 2, 9) + plane, f32),
            pltpu.VMEM((local + 3, 6) + plane, f32),
            pltpu.VMEM((comps,) + plane, f32),
            pltpu.VMEM((SWEEPS, comps) + plane, f32),
            pltpu.VMEM((SWEEPS, comps) + plane, f32),
            pltpu.SemaphoreType.DMA((4,)),
            pltpu.SemaphoreType.DMA((2,)),
            pltpu.SemaphoreType.DMA((SWEEPS + 5,)),
        ],
        compiler_params=pltpu.CompilerParams(collective_id=0, has_side_effects=True),
    )(displacement, load, phase, moduli)
    return pl.pallas_call(
        write_out,
        out_shape=[jax.ShapeDtypeStruct(displacement.shape, f32)] * 2,
        in_specs=[vmem] * 4,
        out_specs=[hbm, hbm],
        scratch_shapes=[pltpu.VMEM((comps,) + plane, f32), pltpu.SemaphoreType.DMA((local + 1,))],
    )(*[pltpu.with_memory_space_constraint(one, pltpu.VMEM) for one in held])


def solution(mesh):
    in_specs = (
        P("slab", None, "rve", None),
        P("slab", None, "rve", None),
        P("slab", "rve", None),
        P(),
    )
    out_specs = (P("slab", None, "rve", None), P("slab", None, "rve", None))
    return jax.shard_map(
        functools.partial(on_device, mesh.shape["slab"]),
        mesh=mesh, in_specs=in_specs, out_specs=out_specs, check_vma=False,
    )
```
